32 devices in a mesh: gx: 4 (over z), gy: 4 (over x, core), gz: 2 (over y).
Axes of the slice: x: 2, y: 2, z: 4, core: 2. Of those that a mesh axis runs over, the one named last changes fastest.
Arguments:
- populations: float32 [19, 16, 32, 512], P(None, 'gz', 'gx', 'gy'), may hold values from 0 to 1, as said below
- omega: float32 [16, 32, 512], P('gz', 'gx', 'gy'), may hold values from 0.8 to 1.7
- obstacle: int32 [16, 32, 512], P('gz', 'gx', 'gy'), may hold values 0 or 1
Outputs:
- lifted: float32 [19, 16, 32, 512], P(None, 'gz', 'gx', 'gy')
- diagnostics: float32 [5], replicated
The draws below stay inside these ranges and needn't reach their ends.
Inputs may be any that keep to these rules, and one draw needn't show every extreme that they name: `populations`: every population lies between 0.3 and 1.7 times its lattice weight.
All inputs are finite; a program needn't handle non-finite values. No bound on the sum of `obstacle` on one device may be relied on, other than what follows from the above.
Results may differ from the reference program's by a relative error of at most 0.0001.
Values sent between devices are 32-bit elements; how exact they have to be, the bound alone decides.
A program may use at most 128 MiB of HBM per device.

```python
import jax
import jax.numpy as jnp

STEPS = 4
JUMP = 2
NX = 32
NY = 512
NZ = 16


def draw_populations(key, part):
    lattice_weights = jnp.array([1.0 / 3.0] + [1.0 / 18.0] * 6 + [1.0 / 36.0] * 12, jnp.float32)[:, None, None, None]
    phases = jax.random.uniform(jax.random.fold_in(key, 7), (3,), jnp.float32, 0.0, 2.0 * jnp.pi)
    zpos = jnp.arange(NZ, dtype=jnp.float32)[None, :, None, None] / NZ
    xpos = jnp.arange(NX, dtype=jnp.float32)[None, None, :, None] / NX
    spread = 0.425 + 0.15 * jnp.sin(2.0 * jnp.pi * zpos + phases[0]) + 0.125 * jnp.sin(2.0 * jnp.pi * xpos + phases[1])
    noise = jax.random.uniform(key, (19, NZ, NX, NY), jnp.float32, -1.0, 1.0)
    return (lattice_weights * (1.0 + spread * noise)).astype(jnp.float32)


def set_ends(drawn, rng, low, high):
    extent = drawn.shape
    index_at = [jax.random.randint(jax.random.fold_in(rng, axis), (), 0, extent[axis]) for axis in range(len(extent))]
    drawn = drawn.at[tuple(index_at)].set(low)
    longest = extent.index(max(extent))
    index_at[longest] = (index_at[longest] + 1) % extent[longest]
    return drawn.at[tuple(index_at)].set(high)


def steps_of(own_key, shape, cuts, least, top_value):
    loudness, own = 1.0, jax.random.fold_in(own_key, 6)
    for dim, parts in cuts:
        heights = jnp.exp(jax.random.uniform(jax.random.fold_in(own, dim), (parts,), jnp.float32, least / len(cuts), top_value / len(cuts)))
        loudness = loudness * jnp.repeat(heights, shape[dim] // parts).reshape([-1 if axis == dim else 1 for axis in range(len(shape))])
    return loudness


def setup_inputs(seed: int = 0) -> dict:
    key_of = jax.random.split(jax.random.key(seed), 4)
    populations = draw_populations(jax.random.fold_in(key_of[3], 71), 0)
    omega = jnp.clip(0.8 + 0.90000004 * jax.random.uniform(key_of[1], (NZ, NX, NY), jnp.float32) ** steps_of(key_of[1], (NZ, NX, NY), ((0, 2), (1, 4), (2, 4)), -0.2, 0.2), 0.8, 1.7)
    obstacle = set_ends((jax.random.randint(key_of[2], (NZ, NX, NY), 0, 8) < 1).astype(jnp.int32), jax.random.fold_in(key_of[2], 1), 0, 1)
    return {"populations": populations, "omega": omega, "obstacle": obstacle}


lattice = [(0, 0, 0), (1, 0, 0), (-1, 0, 0), (0, 1, 0), (0, -1, 0), (0, 0, 1), (0, 0, -1),
           (1, 1, 0), (-1, -1, 0), (1, -1, 0), (-1, 1, 0), (1, 0, 1), (-1, 0, -1), (1, 0, -1), (-1, 0, 1),
           (0, 1, 1), (0, -1, -1), (0, 1, -1), (0, -1, 1)]
weights = [1.0 / 3.0] + [1.0 / 18.0] * 6 + [1.0 / 36.0] * 12
opposite = [0, 2, 1, 4, 3, 6, 5, 8, 7, 10, 9, 12, 11, 14, 13, 16, 15, 18, 17]
limiter = 25.0


def moments(f):
    rho = jnp.sum(f, axis=0)
    comps = []
    for axis_pick in range(3):
        total = jnp.zeros_like(rho)
        for index in range(19):
            comp = lattice[index][axis_pick]
            if comp != 0:
                total = total + comp * f[index]
        comps.append(total)
    return rho, comps[0], comps[1], comps[2]


def equilibrium(rho, momx, momy, momz):
    safe = jnp.maximum(rho, 0.5)
    velx, vely, velz = momx / safe, momy / safe, momz / safe
    square = velx * velx + vely * vely + velz * velz
    rows = []
    for index in range(19):
        cx, cy, cz = lattice[index]
        proj = cx * velx + cy * vely + cz * velz
        rows.append(weights[index] * rho * (1.0 + 3.0 * proj + 4.5 * proj * proj - 1.5 * square))
    return jnp.stack(rows, 0)


def collide(f, omega, solid):
    rho, momx, momy, momz = moments(f)
    feq = equilibrium(rho, momx, momy, momz)
    post = f + omega[None] * (feq - f)
    flipped = jnp.stack([f[opposite[index]] for index in range(19)], 0)
    return jnp.where(solid[None], flipped, post)


def reference(populations, omega, obstacle):
    solid = obstacle == 1
    f = populations
    before = f
    for step in range(STEPS):
        post = collide(f, omega, solid)
        f = jnp.stack([jnp.roll(post[index], (lattice[index][2], lattice[index][0], lattice[index][1]), axis=(0, 1, 2)) for index in range(19)], 0)
        if step == STEPS - 2:
            before = f
    rho_a, jxa, jya, jza = moments(before)
    rho_b, jxb, jyb, jzb = moments(f)
    cells = float(NX * NY * NZ)
    diff_rho = rho_b - rho_a
    diff_x = jxb - jxa
    diff_y = jyb - jya
    diff_z = jzb - jza
    change = jnp.sum(diff_rho * diff_rho + diff_x * diff_x + diff_y * diff_y + diff_z * diff_z) / cells
    gain = JUMP / (1.0 + limiter * change)
    rho_p = rho_b + gain * diff_rho
    jxp = jxb + gain * diff_x
    jyp = jyb + gain * diff_y
    jzp = jzb + gain * diff_z
    lifted = equilibrium(rho_p, jxp, jyp, jzp)
    diagnostics = jnp.stack([change, jnp.sum(jxp) / cells, jnp.sum(jyp) / cells, jnp.sum(jzp) / cells,
                             jnp.sum(jxp * jxp + jyp * jyp + jzp * jzp) / cells])
    return lifted, diagnostics.astype(jnp.float32)
```

```python
import functools

import jax
import jax.numpy as jnp
from jax import lax
from jax.experimental import pallas as pl
from jax.experimental.pallas import tpu as pltpu
from jax.sharding import PartitionSpec as P

STEPS = 4
JUMP = 2
MESH = pl.DeviceIdType.MESH

lattice = [
    (0, 0, 0),
    (1, 0, 0),
    (-1, 0, 0),
    (0, 1, 0),
    (0, -1, 0),
    (0, 0, 1),
    (0, 0, -1),
    (1, 1, 0),
    (-1, -1, 0),
    (1, -1, 0),
    (-1, 1, 0),
    (1, 0, 1),
    (-1, 0, -1),
    (1, 0, -1),
    (-1, 0, 1),
    (0, 1, 1),
    (0, -1, -1),
    (0, 1, -1),
    (0, -1, 1),
]
weights = [1.0 / 3.0] + [1.0 / 18.0] * 6 + [1.0 / 36.0] * 12
limiter = 25.0

slots = [
    (1, 0, -1),
    (1, 0, 0),
    (1, 1, 0),
    (1, -1, 0),
    (1, 0, 1),
    (0, 0, 1),
    (0, 1, 1),
    (0, -1, 1),
    (-1, 0, 1),
    (-1, 0, 0),
    (-1, 1, 0),
    (-1, -1, 0),
    (-1, 0, -1),
    (0, 0, -1),
    (0, 1, -1),
    (0, -1, -1),
    (1, 0, -1),
    (0, 1, 0),
    (0, -1, 0),
    (0, 0, 0),
]
slot_of = {c: i for i, c in enumerate(slots)}
x_first = {1: 0, -1: 8}
z_first = {1: 4, -1: 12}
y_pops = [c for c in lattice if c[1] == 1] + [c for c in lattice if c[1] == -1]
xz_edges = [(1, 0, 1), (-1, 0, 1), (-1, 0, -1), (1, 0, -1)]
xy_edges = [(1, 1, 0), (1, -1, 0), (-1, 1, 0), (-1, -1, 0)]
yz_edges = [(0, 1, 1), (0, -1, 1), (0, 1, -1), (0, -1, -1)]
pairs = [(i, i + 1) for i in range(1, 19, 2)]


def side(sign):
    return 0 if sign == 1 else 1


def moments(f):
    plus = {i: f[i] + f[j] for i, j in pairs}
    minus = {i: f[i] - f[j] for i, j in pairs}
    rho = f[0]
    for i, _ in pairs:
        rho = rho + plus[i]
    comps = []
    for axis in range(3):
        total = None
        for i, _ in pairs:
            c = lattice[i][axis]
            if c:
                term = minus[i]
                total = term * c if total is None else (total + term if c > 0 else total - term)
        comps.append(total)
    return rho, comps


def equilibrium(rho, mom, scale):
    inv = 1.0 / jnp.maximum(rho, 0.5)
    vel = [m * inv for m in mom]
    square = vel[0] * vel[0] + vel[1] * vel[1] + vel[2] * vel[2]
    base = 1.0 - 1.5 * square
    amount = rho if scale is None else scale * rho
    heavy = {w: amount * w for w in sorted(set(weights))}
    rows = [None] * 19
    rows[0] = heavy[weights[0]] * base
    for i, j in pairs:
        proj = None
        for c, v in zip(lattice[i], vel):
            if c:
                proj = (v if c > 0 else -v) if proj is None else (proj + v if c > 0 else proj - v)
        w = heavy[weights[i]]
        even = w * (base + 4.5 * (proj * proj))
        odd = w * (3.0 * proj)
        rows[i] = even + odd
        rows[j] = even - odd
    return rows


def burst_kernel(
    sizes,
    f_hbm,
    omega_hbm,
    obstacle_hbm,
    state_ref,
    diag_ref,
    f_in,
    om_in,
    ob_in,
    post,
    x_send,
    x_recv,
    e_send,
    e_recv,
    c_send,
    c_recv,
    cz_recv,
    moment_a,
    moment_b,
    gathered,
    row_send,
    in_sems,
    send_sems,
    recv_sems,
    sum_send_sems,
    sum_recv_sems,
):
    nx, ny, nz = sizes
    total_devices = nx * ny * nz
    _, Z, X, Y = f_in.shape
    R = X + 16
    gx, gy, gz = (lax.axis_index("gx"), lax.axis_index("gy"), lax.axis_index("gz"))
    me = (gx * ny + gy) * nz + gz

    loads = [
        pltpu.make_async_copy(f_hbm, f_in, in_sems.at[0]),
        pltpu.make_async_copy(omega_hbm, om_in, in_sems.at[1]),
        pltpu.make_async_copy(obstacle_hbm, ob_in, in_sems.at[2]),
    ]
    for load in loads:
        load.start()

    def coords(linear):
        return {"gx": linear // (ny * nz), "gy": (linear // nz) % ny, "gz": linear % nz}

    barrier = pltpu.get_barrier_semaphore()

    def greet(n, carry):
        pl.semaphore_signal(
            barrier, inc=1, device_id=coords((me + n) % total_devices), device_id_type=MESH
        )
        return carry

    lax.fori_loop(1, total_devices, greet, 0)

    lane = lax.broadcasted_iota(jnp.int32, (X, Y), 1)

    def at(z):
        return (z + 1) * R + 8

    def neighbour(offset):
        dx, dy, dz = offset
        return {"gx": (gx + dx + nx) % nx, "gy": (gy + dy + ny) % ny, "gz": (gz + dz + nz) % nz}

    both_z_same = nz == 2

    def messages(s):
        found = []
        for sign in (1, -1):
            rows = pl.ds(at(Z - 1 if sign == 1 else 0), X)
            halo = pl.ds(at(-1 if sign == 1 else Z), X)
            face = pl.ds(z_first[sign], 5)
            found.append((post.at[s, face, rows], post.at[s, face, halo], (0, 0, sign)))
        for sign in (1, -1):
            found.append((x_send.at[s, side(sign)], x_recv.at[s, side(sign)], (sign, 0, 0)))
        for e, c in enumerate(xz_edges):
            found.append((e_send.at[s, e], e_recv.at[s, e], c))
        for sign in (1, -1):
            found.append((c_send.at[s], c_recv.at[s, side(sign), pl.ds(8, X)], (0, sign, 0)))
        for e, c in enumerate(xy_edges):
            row = 4 + side(c[0])
            found.append((e_send.at[s, row], e_recv.at[s, 4 + e], c))
        for e, c in enumerate(yz_edges):
            if both_z_same and c[2] == -1:
                continue
            found.append((c_send.at[s], cz_recv.at[s, e], c))
        return found

    def copies(s):
        return [
            pltpu.make_async_remote_copy(
                src_ref=src,
                dst_ref=dst,
                send_sem=send_sems.at[s, i],
                recv_sem=recv_sems.at[s, i],
                device_id=neighbour(offset),
                device_id_type=MESH,
            )
            for i, (src, dst, offset) in enumerate(messages(s))
        ]

    def collide_plane(s, z, f, packed):
        rho, mom = moments(f)
        for q, value in enumerate([rho] + mom):
            moment_a[q, z] = value
        omega = om_in[z]
        solid = ob_in[z] == 1
        keep = 1.0 - omega
        feq = equilibrium(rho, mom, omega)
        out = {}
        out[0] = jnp.where(solid, f[0], keep * f[0] + feq[0])
        for i, j in pairs:
            out[i] = jnp.where(solid, f[j], keep * f[i] + feq[i])
            out[j] = jnp.where(solid, f[i], keep * f[j] + feq[j])
        by_c = {lattice[i]: out[i] for i in range(19)}
        for k, c in enumerate(slots):
            post[s, k, at(z) : at(z) + X, :] = by_c[c]
        for q, c in enumerate(y_pops):
            k = q * Z + z
            shift = (k + 1) % Y if c[1] == 1 else k
            moved = by_c[c] if shift == 0 else pltpu.roll(by_c[c], shift, 1)
            packed = jnp.where(lane == k, moved, packed)
        return packed

    def send_faces(s, packed):
        for sign in (1, -1):
            row = 8 + (X - 1 if sign == 1 else 0)
            for p in range(5):
                x_send[s, side(sign), p] = post[
                    s, x_first[sign] + p, pl.ds(R + row, Z, stride=R), :
                ]
        for e, (cx, _, cz) in enumerate(xz_edges):
            row = at(Z - 1 if cz == 1 else 0) + (X - 1 if cx == 1 else 0)
            e_send[s, e] = post[s, slot_of[(cx, 0, cz)], pl.ds(row, 1), :]
        c_send[s] = packed
        e_send[s, 4] = packed[X - 1 : X]
        e_send[s, 5] = packed[0:1]
        for copy in copies(s):
            copy.start()

    def receive(s):
        for copy in copies(s):
            copy.wait_recv()
        for sign in (1, -1):
            row = 7 if sign == 1 else X + 8
            for p in range(5):
                post[s, x_first[sign] + p, pl.ds(R + row, Z, stride=R), :] = x_recv[
                    s, side(sign), p
                ]
        for e, (cx, _, cz) in enumerate(xz_edges):
            row = at(-1 if cz == 1 else Z) + (-1 if cx == 1 else X)
            post[s, slot_of[(cx, 0, cz)], pl.ds(row, 1), :] = e_recv[s, e]
        for e, (cx, cy, _) in enumerate(xy_edges):
            row = 7 if cx == 1 else X + 8
            c_recv[s, side(cy), pl.ds(row, 1), :] = e_recv[s, 4 + e]

    def columns(s):
        got = {}
        for sy in (1, -1):
            for cx in (1, 0, -1):
                got[(cx, sy)] = c_recv[s, side(sy), 8 - cx : 8 - cx + X, :]
        for e, c in enumerate(yz_edges):
            slot = yz_edges.index((0, c[1], 1)) if both_z_same else e
            got[c] = cz_recv[s, slot]
        return got

    def stream_plane(s, z, got):
        f = []
        for c in lattice:
            cx, cy, cz = c
            source = z - cz
            slot = slot_of[c]
            if c == (1, 0, -1):
                slot = 0 if source < Z else 16
            row = at(source) - cx
            value = post[s, slot, row : row + X, :]
            if cy:
                outside = source < 0 or source >= Z
                column = got[c] if outside else got[(cx, cy)]
                k = y_pops.index(c) * Z + source % Z
                edge = 0 if cy == 1 else Y - 1
                shift = (edge - k) % Y
                column = column if shift == 0 else pltpu.roll(column, shift, 1)
                value = jnp.where(lane == edge, column, pltpu.roll(value, cy % Y, 1))
            f.append(value)
        return f

    for load in loads:
        load.wait()
    packed = jnp.zeros((X, Y), jnp.float32)
    for z in range(Z):
        packed = collide_plane(0, z, [f_in[i, z] for i in range(19)], packed)
    pl.semaphore_wait(barrier, total_devices - 1)
    send_faces(0, packed)

    def step(s, carry):
        receive(s - 1)
        got = columns(s - 1)
        packed = jnp.zeros((X, Y), jnp.float32)
        for z in range(Z):
            packed = collide_plane(s, z, stream_plane(s - 1, z, got), packed)
        send_faces(s, packed)
        return carry

    lax.fori_loop(1, STEPS, step, 0)
    receive(STEPS - 1)
    got = columns(STEPS - 1)
    sums = [jnp.zeros((X, Y), jnp.float32)] * 10
    for z in range(Z):
        rho, mom = moments(stream_plane(STEPS - 1, z, got))
        now = [rho] + mom
        diff = [now[q] - moment_a[q, z] for q in range(4)]
        for q in range(4):
            moment_b[q, z] = now[q]
            moment_a[q, z] = diff[q]
        terms = [
            diff[0] * diff[0],
            diff[1] * diff[1] + diff[2] * diff[2] + diff[3] * diff[3],
            now[1],
            now[2],
            now[3],
            diff[1],
            diff[2],
            diff[3],
            now[1] * now[1] + now[2] * now[2] + now[3] * now[3],
            now[1] * diff[1] + now[2] * diff[2] + now[3] * diff[3],
        ]
        sums = [a + b for a, b in zip(sums, terms)]

    lane1 = lax.broadcasted_iota(jnp.int32, (1, Y), 1)
    row = jnp.zeros((1, Y), jnp.float32)
    for q, value in enumerate(sums):
        value = jnp.sum(jnp.sum(value, axis=0, keepdims=True), axis=1, keepdims=True)
        row = jnp.where(lane1 == q, value, row)
    row_send[...] = row
    gathered[me] = row

    def share(target, slot):
        return pltpu.make_async_remote_copy(
            src_ref=row_send,
            dst_ref=gathered.at[slot],
            send_sem=sum_send_sems.at[target],
            recv_sem=sum_recv_sems.at[slot],
            device_id=coords(target),
            device_id_type=MESH,
        )

    def share_start(n, carry):
        share((me + n) % total_devices, me).start()
        return carry

    def share_wait(n, carry):
        other = (me + n) % total_devices
        share(other, other).wait_recv()
        return carry

    def share_sent(n, carry):
        share((me + n) % total_devices, me).wait_send()
        return carry

    def steps_sent(s, carry):
        for copy in copies(s):
            copy.wait_send()
        return carry

    lax.fori_loop(1, total_devices, share_start, 0)
    lax.fori_loop(0, STEPS, steps_sent, 0)
    lax.fori_loop(1, total_devices, share_wait, 0)
    total = gathered[0]
    for n in range(1, total_devices):
        total = total + gathered[n]
    lax.fori_loop(1, total_devices, share_sent, 0)

    cells = float(Z * X * Y * total_devices)
    pick = [total[:, q : q + 1] for q in range(10)]
    change = (pick[0] + pick[1]) / cells
    gain = JUMP / (1.0 + limiter * change)
    energy = pick[8] + 2.0 * gain * pick[9] + gain * gain * pick[1]
    diag = [change] + [(pick[2 + a] + gain * pick[5 + a]) / cells for a in range(3)]
    diag.append(energy / cells)
    out = jnp.zeros((1, Y), jnp.float32)
    for q, value in enumerate(diag):
        out = jnp.where(lane1 == q, value, out)
    diag_ref[...] = out
    gains = jnp.broadcast_to(gain, (X, Y))
    for q in range(4):
        for z in range(Z):
            state_ref[q, z] = moment_b[q, z] + gains * moment_a[q, z]


def lift_kernel(state_ref, diag_in, lifted_ref, diag_ref):
    for z in range(state_ref.shape[1]):
        rows = equilibrium(state_ref[0, z], [state_ref[q, z] for q in (1, 2, 3)], None)
        for i in range(19):
            lifted_ref[i, z] = rows[i]
    diag_ref[...] = diag_in[:, 0:5]


def per_device(sizes, populations, omega, obstacle):
    _, Z, X, Y = populations.shape
    R = X + 16
    count = sizes[0] * sizes[1] * sizes[2]
    f32 = jnp.float32
    vmem = pl.BlockSpec(memory_space=pltpu.VMEM)
    hbm = pl.BlockSpec(memory_space=pl.ANY)
    made = 18 if sizes[2] != 2 else 16
    dma = pltpu.SemaphoreType.DMA
    state, diag = pl.pallas_call(
        functools.partial(burst_kernel, sizes),
        out_shape=(
            jax.ShapeDtypeStruct((4, Z, X, Y), f32),
            jax.ShapeDtypeStruct((1, Y), f32),
        ),
        in_specs=[hbm] * 3,
        out_specs=(vmem, vmem),
        scratch_shapes=[
            pltpu.VMEM((19, Z, X, Y), f32),
            pltpu.VMEM((Z, X, Y), f32),
            pltpu.VMEM((Z, X, Y), jnp.int32),
            pltpu.VMEM((STEPS, 20, (Z + 2) * R, Y), f32),
            pltpu.VMEM((STEPS, 2, 5, Z, Y), f32),
            pltpu.VMEM((STEPS, 2, 5, Z, Y), f32),
            pltpu.VMEM((STEPS, 6, 1, Y), f32),
            pltpu.VMEM((STEPS, 8, 1, Y), f32),
            pltpu.VMEM((STEPS, X, Y), f32),
            pltpu.VMEM((STEPS, 2, R, Y), f32),
            pltpu.VMEM((STEPS, 4, X, Y), f32),
            pltpu.VMEM((4, Z, X, Y), f32),
            pltpu.VMEM((4, Z, X, Y), f32),
            pltpu.VMEM((count, 1, Y), f32),
            pltpu.VMEM((1, Y), f32),
            dma((3,)),
            dma((STEPS, made)),
            dma((STEPS, made)),
            dma((count,)),
            dma((count,)),
        ],
        compiler_params=pltpu.CompilerParams(collective_id=0, has_side_effects=True),
    )(populations, omega, obstacle)
    lifted, diag = pl.pallas_call(
        lift_kernel,
        out_shape=(
            jax.ShapeDtypeStruct((19, Z, X, Y), f32),
            jax.ShapeDtypeStruct((1, 5), f32),
        ),
        in_specs=[vmem, vmem],
        out_specs=(vmem, vmem),
    )(state, diag)
    return lifted, diag.reshape(5)


def solution(mesh):
    in_specs = (P(None, "gz", "gx", "gy"), P("gz", "gx", "gy"), P("gz", "gx", "gy"))
    out_specs = (P(None, "gz", "gx", "gy"), P())
    sizes = (mesh.shape["gx"], mesh.shape["gy"], mesh.shape["gz"])
    return jax.shard_map(
        functools.partial(per_device, sizes),
        mesh=mesh,
        in_specs=in_specs,
        out_specs=out_specs,
        check_vma=False,
    )
```
